16 devices in a mesh: fsdp: 2 (over z), ep: 8 (over y, x, core).
Axes of the slice: x: 2, y: 2, z: 2, core: 2. Of those that a mesh axis runs over, the one named last changes fastest.
Arguments:
- layer_in: bfloat16 [32768, 1536], P(('fsdp', 'ep'))
- out_grad: bfloat16 [32768, 1536], P(('fsdp', 'ep'))
- expert_ids: int32 [32768, 8], P(('fsdp', 'ep'))
- gate_vals: float32 [32768, 8], P(('fsdp', 'ep'))
- w_one: bfloat16 [40, 1536, 512], P('ep', 'fsdp')
- w_two: bfloat16 [40, 512, 1536], P('ep', None, 'fsdp')
- w_three: bfloat16 [40, 1536, 512], P('ep', 'fsdp')
Outputs:
- output 1: bfloat16 [32768, 1536], P(('fsdp', 'ep'))
- output 2: float32 [32768, 8], P(('fsdp', 'ep'))
- output 3: float32 [40, 1536, 512], P('ep', 'fsdp')
- output 4: float32 [40, 512, 1536], P('ep', None, 'fsdp')
- output 5: float32 [40, 1536, 512], P('ep', 'fsdp')
All inputs are finite; a program needn't handle non-finite values.
Results may differ from the reference program's by a relative error of at most 0.00144.
Values are sent between devices in bfloat16 or wider.
A program may use at most 1 GiB of HBM per device.

```python
import jax
import jax.numpy as jnp
from jax import lax

HIDDEN = 1536
EXPERT_FF = 512
EXPERTS = 40
TOP_K = 8
TOKENS_DEV = 2048
SHARDS = 16
CAPACITY = 512
TOKENS = SHARDS * TOKENS_DEV


def draw_routing(key):
    key_bias, key_hot, key_noise = jax.random.split(key, 3)
    noise_range = 65536
    spread = noise_range * TOP_K // (2 * EXPERTS)
    bias = jax.random.randint(key_bias, (EXPERTS,), 0, spread + 1)
    hot_expert = jax.random.randint(key_hot, (), 0, EXPERTS)
    expert_pos = jnp.arange(EXPERTS, dtype=jnp.int32)
    bias = bias + jnp.where(expert_pos == hot_expert, noise_range // 4, 0)
    noise = jax.random.randint(key_noise, (TOKENS, EXPERTS), 0, noise_range)
    scores = (noise + bias[None, :]) * EXPERTS + expert_pos[None, :]
    return lax.top_k(scores, TOP_K)[1].astype(jnp.int32)


def setup_inputs(seed: int = 0) -> dict:
    keys = jax.random.split(jax.random.key(seed), 7)
    layer_in = jax.random.normal(keys[0], (TOKENS, HIDDEN), jnp.float32).astype(jnp.bfloat16)
    out_grad = jax.random.normal(keys[1], (TOKENS, HIDDEN), jnp.float32).astype(jnp.bfloat16)
    expert_ids = draw_routing(keys[2])
    gate_vals = jax.random.uniform(keys[3], (TOKENS, TOP_K), jnp.float32, 0.25, 1.0)
    w_one = (jax.random.normal(keys[4], (EXPERTS, HIDDEN, EXPERT_FF), jnp.float32) * HIDDEN ** -0.5).astype(jnp.bfloat16)
    w_two = (jax.random.normal(keys[5], (EXPERTS, EXPERT_FF, HIDDEN), jnp.float32) * EXPERT_FF ** -0.5).astype(jnp.bfloat16)
    w_three = (jax.random.normal(keys[6], (EXPERTS, HIDDEN, EXPERT_FF), jnp.float32) * HIDDEN ** -0.5).astype(jnp.bfloat16)
    return {"layer_in": layer_in, "out_grad": out_grad, "expert_ids": expert_ids, "gate_vals": gate_vals, "w_one": w_one, "w_two": w_two, "w_three": w_three}


def reference(layer_in, out_grad, expert_ids, gate_vals, w_one, w_two, w_three):
    w_one_full = w_one.astype(jnp.float32)
    w_two_full = w_two.astype(jnp.float32)
    w_three_full = w_three.astype(jnp.float32)
    places = EXPERTS * CAPACITY
    expert_pos = jnp.arange(EXPERTS, dtype=jnp.int32)
    token_of = jnp.arange(TOKENS_DEV * TOP_K, dtype=jnp.int32) // TOP_K

    def shard_step(carry, shard):
        x_loc, dy_loc, ids_loc, gates_loc = shard
        flat_ids = ids_loc.reshape(-1)
        onehot = (flat_ids[:, None] == expert_pos[None, :]).astype(jnp.int32)
        before = jnp.cumsum(onehot, axis=0) - onehot
        position = jnp.sum(before * onehot, axis=1)
        slot_of = jnp.where(position < CAPACITY, flat_ids * CAPACITY + position, places)
        source = jnp.full((places,), TOKENS_DEV, jnp.int32).at[slot_of].set(token_of, mode="drop")
        slot_gate = jnp.zeros((places,), jnp.float32).at[slot_of].set(gates_loc.reshape(-1), mode="drop")
        x_buf = jnp.take(x_loc, source, axis=0, mode="fill", fill_value=0).reshape(EXPERTS, CAPACITY, HIDDEN).astype(jnp.float32)
        dy_buf = jnp.take(dy_loc, source, axis=0, mode="fill", fill_value=0).reshape(EXPERTS, CAPACITY, HIDDEN).astype(jnp.float32)
        h_one = jnp.einsum("ecd,edf->ecf", x_buf, w_one_full)
        h_three = jnp.einsum("ecd,edf->ecf", x_buf, w_three_full)
        sig_one = jax.nn.sigmoid(h_one)
        silu_one = h_one * sig_one
        act_bf = (silu_one * h_three).astype(jnp.bfloat16).astype(jnp.float32)
        y_buf = jnp.einsum("ecf,efd->ecd", act_bf, w_two_full)
        gate_buf = jnp.sum(dy_buf * y_buf, axis=-1)
        g_buf = (slot_gate.reshape(EXPERTS, CAPACITY, 1) * dy_buf).astype(jnp.bfloat16).astype(jnp.float32)
        d_act = jnp.einsum("ecd,efd->ecf", g_buf, w_two_full)
        dh_one = (d_act * h_three * sig_one * (1.0 + h_one * (1.0 - sig_one))).astype(jnp.bfloat16).astype(jnp.float32)
        dh_three = (d_act * silu_one).astype(jnp.bfloat16).astype(jnp.float32)
        dx_buf = (jnp.einsum("ecf,edf->ecd", dh_one, w_one_full) + jnp.einsum("ecf,edf->ecd", dh_three, w_three_full)).astype(jnp.bfloat16)
        dx_pick = jnp.take(dx_buf.reshape(places, HIDDEN), slot_of, axis=0, mode="fill", fill_value=0).reshape(TOKENS_DEV, TOP_K, HIDDEN)
        dx_tok = jnp.sum(dx_pick.astype(jnp.float32), axis=1).astype(jnp.bfloat16)
        gate_tok = jnp.take(gate_buf.reshape(places), slot_of, axis=0, mode="fill", fill_value=0).reshape(TOKENS_DEV, TOP_K)
        acc_one, acc_two, acc_three = carry
        acc_one = acc_one + jnp.einsum("ecd,ecf->edf", x_buf, dh_one)
        acc_two = acc_two + jnp.einsum("ecf,ecd->efd", act_bf, g_buf)
        acc_three = acc_three + jnp.einsum("ecd,ecf->edf", x_buf, dh_three)
        return (acc_one, acc_two, acc_three), (dx_tok, gate_tok)

    init = (jnp.zeros((EXPERTS, HIDDEN, EXPERT_FF), jnp.float32), jnp.zeros((EXPERTS, EXPERT_FF, HIDDEN), jnp.float32), jnp.zeros((EXPERTS, HIDDEN, EXPERT_FF), jnp.float32))
    shards = (layer_in.reshape(SHARDS, TOKENS_DEV, HIDDEN), out_grad.reshape(SHARDS, TOKENS_DEV, HIDDEN), expert_ids.reshape(SHARDS, TOKENS_DEV, TOP_K), gate_vals.reshape(SHARDS, TOKENS_DEV, TOP_K))
    (grad_one, grad_two, grad_three), (in_grad, gate_grad) = lax.scan(shard_step, init, shards)
    return in_grad.reshape(TOKENS, HIDDEN), gate_grad.reshape(TOKENS, TOP_K), grad_one, grad_two, grad_three
```

```python
import functools

import jax
import jax.numpy as jnp
from jax import lax
from jax.experimental import pallas as pl
from jax.experimental.pallas import tpu as pltpu
from jax.sharding import PartitionSpec as P

F32, BF16, I32 = jnp.float32, jnp.bfloat16, jnp.int32
COL_CHUNKS = 2
TOKENS = 256
IN_WINDOW = 96
OUT_WINDOW = 128
ALIGN = 16


def capacity_of(tok_dev, top_k, experts):
    return max(8, ((tok_dev * top_k * 5) // (4 * experts) + 7) // 8 * 8)


def route(ids_all, gates_all, first_expert, local_experts, capacity):
    ids_t = jnp.swapaxes(ids_all, 1, 2)
    gates_t = jnp.swapaxes(gates_all, 1, 2)
    mine = first_expert + jnp.arange(local_experts, dtype=I32)
    match = ids_t[:, None] == mine[None, :, None, None]
    hit = jnp.any(match, axis=2).astype(I32)
    gate_te = jnp.sum(jnp.where(match, gates_t[:, None], 0.0), axis=2)
    upto = jnp.cumsum(hit, axis=-1)
    place = jnp.where((hit > 0) & (upto <= capacity), upto - 1, -1)
    ends = jnp.minimum(upto[:, :, TOKENS - 1 :: TOKENS], capacity)
    starts = jnp.concatenate([jnp.zeros_like(ends[:, :, :1]), ends[:, :, :-1]], axis=-1)
    starts = starts // ALIGN * ALIGN
    return place, gate_te, jnp.swapaxes(starts, 1, 2), jnp.swapaxes(ends, 1, 2)


def rounds_of(starts, ends, window):
    return jnp.max((ends - starts + window - 1) // window, axis=-1)


def gather_kernel(local_experts, capacity, cols, with_gate, starts, rounds, place_ref, gate_ref, x_ref, *outs):
    src, blk = pl.program_id(0), pl.program_id(1)
    blocks = pl.num_programs(1)
    step = src * blocks + blk
    hidden = x_ref.shape[-1]
    W = IN_WINDOW

    @pl.when(blk == 0)
    def _():
        for out in outs:
            for e in range(local_experts):
                out[0, e] = jnp.zeros(out.shape[2:], out.dtype)

    def one_round(r, carry):
        picks, gates, bases = [], [], []
        for e in range(local_experts):
            low = starts[step * local_experts + e] + r * W
            base = pl.multiple_of(jnp.minimum(low, capacity - W), ALIGN)
            slot = base + lax.broadcasted_iota(I32, (W, TOKENS), 0)
            hit = (place_ref[0, e:e + 1, :] == slot) & (slot >= low)
            picks.append(jnp.where(hit, 1.0, 0.0).astype(BF16))
            if with_gate:
                gates.append(jnp.sum(jnp.where(hit, gate_ref[0, e:e + 1, :], 0.0), axis=1, keepdims=True))
            bases.append(base)
        pick = jnp.concatenate(picks, axis=0)
        for c in range(0, hidden, cols):
            rows = jnp.dot(pick, x_ref[:, c:c + cols], preferred_element_type=F32)
            for e in range(local_experts):
                part = rows[e * W:(e + 1) * W]
                at = (0, e, pl.ds(bases[e], W), slice(c, c + cols))
                outs[0][at] = outs[0][at] + part.astype(BF16)
                if with_gate:
                    outs[1][at] = outs[1][at] + (gates[e] * part).astype(BF16)
        return carry

    lax.fori_loop(0, rounds[step], one_round, 0)


def gather_rows(x_all, place8, gate8, starts, ends, local_experts, capacity, with_gate):
    sources, _, tok_dev = place8.shape
    hidden = x_all.shape[-1]
    blocks = tok_dev // TOKENS
    rounds = rounds_of(starts, ends, IN_WINDOW).reshape(-1)
    shape = jax.ShapeDtypeStruct((sources, local_experts, capacity, hidden), BF16)
    out_spec = pl.BlockSpec((1, local_experts, capacity, hidden), lambda s, b, *_: (s, 0, 0, 0))
    row_spec = pl.BlockSpec((1, 8, TOKENS), lambda s, b, *_: (s, 0, b))
    n_out = 2 if with_gate else 1
    places = sources * local_experts * capacity
    out = pl.pallas_call(
        functools.partial(gather_kernel, local_experts, capacity, 512 if hidden % 512 == 0 else hidden, with_gate),
        grid_spec=pltpu.PrefetchScalarGridSpec(
            num_scalar_prefetch=2,
            grid=(sources, blocks),
            in_specs=[row_spec, row_spec, pl.BlockSpec((TOKENS, hidden), lambda s, b, *_: (s * blocks + b, 0))],
            out_specs=[out_spec] * n_out,
        ),
        out_shape=[shape] * n_out,
        cost_estimate=pl.CostEstimate(flops=2 * places * 512 * hidden, bytes_accessed=2 * hidden * (sources * tok_dev + n_out * places), transcendentals=0),
        compiler_params=pltpu.CompilerParams(dimension_semantics=("arbitrary", "arbitrary"), vmem_limit_bytes=56 << 20),
        name="gather_rows",
    )(starts.reshape(-1), rounds, place8, gate8, x_all)
    return out


def nt_dot(a, b):
    return lax.dot_general(a, b, (((1,), (1,)), ((), ())), preferred_element_type=F32)


def combine_kernel(local_experts, capacity, starts, rounds, place_ref, dh1_ref, dh3_ref, w1_ref, w3_ref, out_ref, dx_ref):
    src = pl.program_id(0)
    blocks = out_ref.shape[1] // TOKENS
    W = OUT_WINDOW
    tile = 256 if capacity % 256 == 0 else capacity
    tiles = capacity // tile

    def one_tile(i, carry):
        e, m = i // tiles, i % tiles
        rows = pl.ds(pl.multiple_of(m * tile, tile), tile)
        dx = nt_dot(dh1_ref[0, e, rows, :], w1_ref[e]) + nt_dot(dh3_ref[0, e, rows, :], w3_ref[e])
        dx_ref[e, rows, :] = dx.astype(BF16)
        return carry

    lax.fori_loop(0, local_experts * tiles, one_tile, 0)

    def one_block(b, carry):
        step = src * blocks + b
        toks = pl.ds(pl.multiple_of(b * TOKENS, TOKENS), TOKENS)
        place = place_ref[0, toks, :]

        def part(r):
            picks, rows = [], []
            for e in range(local_experts):
                low = starts[step * local_experts + e] + r * W
                base = pl.multiple_of(jnp.minimum(low, capacity - W), ALIGN)
                slot = base + lax.broadcasted_iota(I32, (TOKENS, W), 1)
                hit = (place[:, e:e + 1] == slot) & (slot >= low)
                picks.append(jnp.where(hit, 1.0, 0.0).astype(BF16))
                rows.append(dx_ref[e, pl.ds(base, W), :])
            return jnp.dot(jnp.concatenate(picks, axis=1), jnp.concatenate(rows, axis=0), preferred_element_type=F32)

        out_ref[0, toks, :] = part(0)

        def more(r, c):
            out_ref[0, toks, :] += part(r)
            return c

        lax.fori_loop(1, rounds[step], more, 0)
        return carry

    lax.fori_loop(0, blocks, one_block, 0)


def combine_rows(dh1, dh3, w1, w3, place_t, starts, ends, chunk, cols):
    sources, local_experts, capacity, ff = dh1.shape
    tok_dev = place_t.shape[1]
    rounds = rounds_of(starts, ends, OUT_WINDOW).reshape(-1)
    dh_spec = pl.BlockSpec((1, local_experts, capacity, ff), lambda s, *_: (s, 0, 0, 0))
    w_spec = pl.BlockSpec((local_experts, cols, ff), lambda s, *_: (0, chunk, 0))
    places = sources * local_experts * capacity
    return pl.pallas_call(
        functools.partial(combine_kernel, local_experts, capacity),
        grid_spec=pltpu.PrefetchScalarGridSpec(
            num_scalar_prefetch=2,
            grid=(sources,),
            in_specs=[pl.BlockSpec((1, tok_dev, 8), lambda s, *_: (s, 0, 0)), dh_spec, dh_spec, w_spec, w_spec],
            out_specs=pl.BlockSpec((1, tok_dev, cols), lambda s, *_: (s, 0, 0)),
            scratch_shapes=[pltpu.VMEM((local_experts, capacity, cols), BF16)],
        ),
        out_shape=jax.ShapeDtypeStruct((sources, tok_dev, cols), F32),
        cost_estimate=pl.CostEstimate(flops=2 * places * cols * (2 * ff + 512), bytes_accessed=4 * sources * tok_dev * cols + 4 * places * ff, transcendentals=0),
        compiler_params=pltpu.CompilerParams(dimension_semantics=("arbitrary",), vmem_limit_bytes=58 << 20),
        name="combine_rows",
    )(starts.reshape(-1), rounds, place_t, dh1, dh3, w1, w3)


def fsdp_full(part, other, pos, axis):
    size = part.shape[axis]
    shape = part.shape[:axis] + (2 * size,) + part.shape[axis + 1:]
    full = lax.dynamic_update_slice_in_dim(jnp.zeros(shape, part.dtype), part, pos * size, axis)
    return lax.dynamic_update_slice_in_dim(full, other, (1 - pos) * size, axis)


def dot(spec, a, b):
    return jnp.einsum(spec, a, b, preferred_element_type=F32)


def solution(mesh):
    ep_size = mesh.shape["ep"]
    tok_spec = P(("fsdp", "ep"), None)
    up_spec = P("ep", "fsdp", None)
    down_spec = P("ep", None, "fsdp")
    swap = [(0, 1), (1, 0)]

    def per_device(layer_in, out_grad, expert_ids, gate_vals, w_one, w_two, w_three):
        tok_dev, hidden = layer_in.shape
        top_k = expert_ids.shape[1]
        local_experts = w_one.shape[0]
        experts = local_experts * ep_size
        capacity = capacity_of(tok_dev, top_k, experts)
        fpos = lax.axis_index("fsdp")
        epos = lax.axis_index("ep")
        ids_all = lax.all_gather(expert_ids, "ep")
        gates_all = lax.all_gather(gate_vals, "ep")
        x_all = lax.all_gather(layer_in, "ep", tiled=True)
        u_all = lax.all_gather(out_grad, "ep", tiled=True)
        w1 = fsdp_full(w_one, lax.ppermute(w_one, "fsdp", swap), fpos, 1)
        w3 = fsdp_full(w_three, lax.ppermute(w_three, "fsdp", swap), fpos, 1)
        w2 = fsdp_full(w_two, lax.ppermute(w_two, "fsdp", swap), fpos, 2)
        place, gate_te, starts, ends = route(ids_all, gates_all, epos * local_experts, local_experts, capacity)
        pad = ((0, 0), (0, 8 - local_experts), (0, 0))
        place8 = jnp.pad(place, pad, constant_values=-1)
        gate8 = jnp.pad(gate_te, pad)
        place_t = jnp.swapaxes(place8, 1, 2)

        def over_fsdp(grad, axis):
            size = grad.shape[axis] // 2
            away = lax.dynamic_slice_in_dim(grad, (1 - fpos) * size, size, axis)
            keep = lax.dynamic_slice_in_dim(grad, fpos * size, size, axis)
            return keep, lax.ppermute(away, "fsdp", swap)

        x_rows, = gather_rows(x_all, place8, gate8, starts, ends, local_experts, capacity, False)
        h1 = dot("pecd,edf->pecf", x_rows, w1)
        h3 = dot("pecd,edf->pecf", x_rows, w3)
        sig = jax.nn.sigmoid(h1)
        silu = h1 * sig
        act = (silu * h3).astype(BF16)
        u_rows, g_rows = gather_rows(u_all, place8, gate8, starts, ends, local_experts, capacity, True)
        grad2 = dot("pecf,pecd->efd", act, g_rows)
        g_rows, grad2 = lax.optimization_barrier((g_rows, grad2))
        keep2, other2 = over_fsdp(grad2, 2)
        da = dot("pecd,efd->pecf", g_rows, w2)
        dh1 = (da * h3 * sig * (1.0 + h1 * (1.0 - sig))).astype(BF16)
        dh3 = (da * silu).astype(BF16)

        cols = hidden // COL_CHUNKS
        dx_parts = []
        for c in range(COL_CHUNKS):
            part = combine_rows(dh1, dh3, w1, w3, place_t, starts, ends, c, cols)
            dx_parts.append(lax.psum_scatter(part, "ep", scatter_dimension=0, tiled=True)[0].astype(BF16))
        in_grad = jnp.concatenate(dx_parts, axis=-1)

        grad1 = dot("pecd,pecf->edf", x_rows, dh1)
        keep1, other1 = over_fsdp(grad1, 1)
        grad3 = dot("pecd,pecf->edf", x_rows, dh3)
        keep3, other3 = over_fsdp(grad3, 1)

        v = dot("pecd,efd->pecf", u_rows, w2)
        slot_dgate = jnp.sum(act.astype(F32) * v, axis=-1)
        spots = jnp.arange(capacity, dtype=I32)
        dense = jnp.sum(jnp.where(place[..., None] == spots, slot_dgate[:, :, None, :], 0.0), axis=-1)
        back = lax.all_to_all(dense, "ep", 0, 0, tiled=True).reshape(experts, tok_dev)
        every = jnp.arange(experts, dtype=I32)[:, None, None]
        gate_out = jnp.sum(jnp.where(expert_ids[None] == every, back[..., None], 0.0), axis=0)
        return in_grad, gate_out, keep1 + other1, keep2 + other2, keep3 + other3

    return jax.shard_map(per_device, mesh=mesh, in_specs=(tok_spec, tok_spec, tok_spec, tok_spec, up_spec, down_spec, up_spec), out_specs=(tok_spec, tok_spec, up_spec, down_spec, up_spec), check_vma=False)
```

```python
import functools

import jax
import jax.numpy as jnp
from jax import lax
from jax.experimental import pallas as pl
from jax.experimental.pallas import tpu as pltpu
from jax.sharding import PartitionSpec as P


F32, BF16, I32 = jnp.float32, jnp.bfloat16, jnp.int32
TOKENS = 256
IN_WINDOW = 96
OUT_WINDOW = 128
ALIGN = 16


def capacity_of(tok_dev, top_k, experts):
    return max(8, ((tok_dev * top_k * 5) // (4 * experts) + 7) // 8 * 8)


def route(ids_all, gates_all, first_expert, local_experts, capacity):
    ids_t = jnp.swapaxes(ids_all, 1, 2)
    gates_t = jnp.swapaxes(gates_all, 1, 2)
    mine = first_expert + jnp.arange(local_experts, dtype=I32)
    match = ids_t[:, None] == mine[None, :, None, None]
    hit = jnp.any(match, axis=2).astype(I32)
    gate_te = jnp.sum(jnp.where(match, gates_t[:, None], 0.0), axis=2)
    upto = jnp.cumsum(hit, axis=-1)
    place = jnp.where((hit > 0) & (upto <= capacity), upto - 1, -1)
    ends = jnp.minimum(upto[:, :, TOKENS - 1 :: TOKENS], capacity)
    starts = jnp.concatenate([jnp.zeros_like(ends[:, :, :1]), ends[:, :, :-1]], axis=-1)
    starts = starts // ALIGN * ALIGN
    return place, gate_te, jnp.swapaxes(starts, 1, 2), jnp.swapaxes(ends, 1, 2)


def rounds_of(starts, ends, window):
    return jnp.max((ends - starts + window - 1) // window, axis=-1)


def gather_kernel(local_experts, capacity, cols, with_gate, starts, rounds, place_ref, gate_ref, x_ref, *outs):
    src, blk = pl.program_id(0), pl.program_id(1)
    blocks = pl.num_programs(1)
    step = src * blocks + blk
    hidden = x_ref.shape[-1]
    W = IN_WINDOW

    @pl.when(blk == 0)
    def _():
        for out in outs:
            for e in range(local_experts):
                out[0, e] = jnp.zeros(out.shape[2:], out.dtype)

    def one_round(r, carry):
        picks, gates, bases = [], [], []
        for e in range(local_experts):
            low = starts[step * local_experts + e] + r * W
            base = pl.multiple_of(jnp.minimum(low, capacity - W), ALIGN)
            slot = base + lax.broadcasted_iota(I32, (W, TOKENS), 0)
            hit = (place_ref[0, e:e + 1, :] == slot) & (slot >= low)
            picks.append(jnp.where(hit, 1.0, 0.0).astype(BF16))
            if with_gate:
                gates.append(jnp.sum(jnp.where(hit, gate_ref[0, e:e + 1, :], 0.0), axis=1, keepdims=True))
            bases.append(base)
        pick = jnp.concatenate(picks, axis=0)
        for c in range(0, hidden, cols):
            rows = jnp.dot(pick, x_ref[:, c:c + cols], preferred_element_type=F32)
            for e in range(local_experts):
                part = rows[e * W:(e + 1) * W]
                at = (0, e, pl.ds(bases[e], W), slice(c, c + cols))
                outs[0][at] = outs[0][at] + part.astype(BF16)
                if with_gate:
                    outs[1][at] = outs[1][at] + (gates[e] * part).astype(BF16)
        return carry

    lax.fori_loop(0, rounds[step], one_round, 0)


def gather_rows(x_all, place8, gate8, starts, ends, local_experts, capacity, with_gate):
    sources, _, tok_dev = place8.shape
    hidden = x_all.shape[-1]
    blocks = tok_dev // TOKENS
    rounds = rounds_of(starts, ends, IN_WINDOW).reshape(-1)
    shape = jax.ShapeDtypeStruct((sources, local_experts, capacity, hidden), BF16)
    out_spec = pl.BlockSpec((1, local_experts, capacity, hidden), lambda s, b, *_: (s, 0, 0, 0))
    row_spec = pl.BlockSpec((1, 8, TOKENS), lambda s, b, *_: (s, 0, b))
    n_out = 2 if with_gate else 1
    places = sources * local_experts * capacity
    out = pl.pallas_call(
        functools.partial(gather_kernel, local_experts, capacity, 512 if hidden % 512 == 0 else hidden, with_gate),
        grid_spec=pltpu.PrefetchScalarGridSpec(
            num_scalar_prefetch=2,
            grid=(sources, blocks),
            in_specs=[row_spec, row_spec, pl.BlockSpec((TOKENS, hidden), lambda s, b, *_: (s * blocks + b, 0))],
            out_specs=[out_spec] * n_out,
        ),
        out_shape=[shape] * n_out,
        cost_estimate=pl.CostEstimate(flops=2 * places * 512 * hidden, bytes_accessed=2 * hidden * (sources * tok_dev + n_out * places), transcendentals=0),
        compiler_params=pltpu.CompilerParams(dimension_semantics=("arbitrary", "arbitrary"), vmem_limit_bytes=56 << 20),
        name="gather_rows",
    )(starts.reshape(-1), rounds, place8, gate8, x_all)
    return out


def nt_dot(a, b):
    return lax.dot_general(a, b, (((1,), (1,)), ((), ())), preferred_element_type=F32)


def combine_kernel(local_experts, capacity, starts, rounds, place_ref, dh1_ref, dh3_ref, w1_ref, w3_ref, out_ref, dx_ref):
    src = pl.program_id(0)
    blocks = out_ref.shape[1] // TOKENS
    W = OUT_WINDOW
    tile = 256 if capacity % 256 == 0 else capacity
    tiles = capacity // tile

    def one_tile(i, carry):
        e, m = i // tiles, i % tiles
        rows = pl.ds(pl.multiple_of(m * tile, tile), tile)
        dx = nt_dot(dh1_ref[0, e, rows, :], w1_ref[e]) + nt_dot(dh3_ref[0, e, rows, :], w3_ref[e])
        dx_ref[e, rows, :] = dx.astype(BF16)
        return carry

    lax.fori_loop(0, local_experts * tiles, one_tile, 0)

    def one_block(b, carry):
        step = src * blocks + b
        toks = pl.ds(pl.multiple_of(b * TOKENS, TOKENS), TOKENS)
        place = place_ref[0, toks, :]

        def part(r):
            picks, rows = [], []
            for e in range(local_experts):
                low = starts[step * local_experts + e] + r * W
                base = pl.multiple_of(jnp.minimum(low, capacity - W), ALIGN)
                slot = base + lax.broadcasted_iota(I32, (TOKENS, W), 1)
                hit = (place[:, e:e + 1] == slot) & (slot >= low)
                picks.append(jnp.where(hit, 1.0, 0.0).astype(BF16))
                rows.append(dx_ref[e, pl.ds(base, W), :])
            return jnp.dot(jnp.concatenate(picks, axis=1), jnp.concatenate(rows, axis=0), preferred_element_type=F32)

        out_ref[0, toks, :] = part(0)

        def more(r, c):
            out_ref[0, toks, :] += part(r)
            return c

        lax.fori_loop(1, rounds[step], more, 0)
        return carry

    lax.fori_loop(0, blocks, one_block, 0)


def combine_rows(dh1, dh3, w1, w3, place_t, starts, ends, chunk, cols):
    sources, local_experts, capacity, ff = dh1.shape
    tok_dev = place_t.shape[1]
    rounds = rounds_of(starts, ends, OUT_WINDOW).reshape(-1)
    dh_spec = pl.BlockSpec((1, local_experts, capacity, ff), lambda s, *_: (s, 0, 0, 0))
    w_spec = pl.BlockSpec((local_experts, cols, ff), lambda s, *_: (0, chunk, 0))
    places = sources * local_experts * capacity
    return pl.pallas_call(
        functools.partial(combine_kernel, local_experts, capacity),
        grid_spec=pltpu.PrefetchScalarGridSpec(
            num_scalar_prefetch=2,
            grid=(sources,),
            in_specs=[pl.BlockSpec((1, tok_dev, 8), lambda s, *_: (s, 0, 0)), dh_spec, dh_spec, w_spec, w_spec],
            out_specs=pl.BlockSpec((1, tok_dev, cols), lambda s, *_: (s, 0, 0)),
            scratch_shapes=[pltpu.VMEM((local_experts, capacity, cols), BF16)],
        ),
        out_shape=jax.ShapeDtypeStruct((sources, tok_dev, cols), F32),
        cost_estimate=pl.CostEstimate(flops=2 * places * cols * (2 * ff + 512), bytes_accessed=4 * sources * tok_dev * cols + 4 * places * ff, transcendentals=0),
        compiler_params=pltpu.CompilerParams(dimension_semantics=("arbitrary",), vmem_limit_bytes=58 << 20),
        name="combine_rows",
    )(starts.reshape(-1), rounds, place_t, dh1, dh3, w1, w3)


def fsdp_full(part, other, pos, axis):
    size = part.shape[axis]
    shape = part.shape[:axis] + (2 * size,) + part.shape[axis + 1:]
    full = lax.dynamic_update_slice_in_dim(jnp.zeros(shape, part.dtype), part, pos * size, axis)
    return lax.dynamic_update_slice_in_dim(full, other, (1 - pos) * size, axis)


def dot(spec, a, b):
    return jnp.einsum(spec, a, b, preferred_element_type=F32)


def solution(mesh):
    ep_size = mesh.shape["ep"]
    tok_spec = P(("fsdp", "ep"), None)
    up_spec = P("ep", "fsdp", None)
    down_spec = P("ep", None, "fsdp")
    swap = [(0, 1), (1, 0)]

    def body(layer_in, out_grad, expert_ids, gate_vals, w_one, w_two, w_three):
        tok_dev, hidden = layer_in.shape
        top_k = expert_ids.shape[1]
        local_experts = w_one.shape[0]
        experts = local_experts * ep_size
        capacity = capacity_of(tok_dev, top_k, experts)
        fpos = lax.axis_index("fsdp")
        epos = lax.axis_index("ep")
        half = hidden // 2
        ids_all = lax.all_gather(expert_ids, "ep")
        gates_all = lax.all_gather(gate_vals, "ep")
        x_all = lax.all_gather(layer_in, "ep", tiled=True)
        w_one_other = lax.ppermute(w_one, "fsdp", swap)
        w_three_other = lax.ppermute(w_three, "fsdp", swap)
        w_two_other = lax.ppermute(w_two, "fsdp", swap)
        w2a = jnp.where(fpos == 0, w_two, w_two_other)
        w2b = jnp.where(fpos == 0, w_two_other, w_two)
        place, gate_te, starts, ends = route(ids_all, gates_all, epos * local_experts, local_experts, capacity)
        pad = ((0, 0), (0, 8 - local_experts), (0, 0))
        place8 = jnp.pad(place, pad, constant_values=-1)
        gate8 = jnp.pad(gate_te, pad)
        low, high, x_all, w_one_other, w_three_other, place8, gate8, starts, ends = lax.optimization_barrier((out_grad[:, :half], out_grad[:, half:], x_all, w_one_other, w_three_other, place8, gate8, starts, ends))
        place_t = jnp.swapaxes(place8, 1, 2)
        w1 = fsdp_full(w_one, w_one_other, fpos, 1)
        w3 = fsdp_full(w_three, w_three_other, fpos, 1)
        u_all_a = lax.all_gather(low, "ep", tiled=True)
        high, x_rows = lax.optimization_barrier((high, gather_rows(x_all, place8, gate8, starts, ends, local_experts, capacity, False)[0]))
        u_all_b = lax.all_gather(high, "ep", tiled=True)

        def pick(rows, with_gate):
            return gather_rows(rows, place8, gate8, starts, ends, local_experts, capacity, with_gate)

        def over_fsdp(low, high):
            return jnp.where(fpos == 0, low, high), jnp.where(fpos == 0, high, low)

        h1 = dot("pecd,edf->pecf", x_rows, w1)
        h3 = dot("pecd,edf->pecf", x_rows, w3)
        sig = jax.nn.sigmoid(h1)
        silu = h1 * sig
        act = (silu * h3).astype(BF16)
        u_a, g_a = pick(u_all_a, True)
        da_a = dot("pecd,efd->pecf", g_a, w2a)
        u_all_b, da_a = lax.optimization_barrier((u_all_b, da_a))
        u_b, g_b = pick(u_all_b, True)
        da = da_a + dot("pecd,efd->pecf", g_b, w2b)
        dh1 = (da * h3 * sig * (1.0 + h1 * (1.0 - sig))).astype(BF16)
        dh3 = (da * silu).astype(BF16)

        def combine(d1, d3, cols, at):
            return combine_rows(d1, d3, w1, w3, place_t, starts, ends, at, cols)

        def spread(part):
            return lax.psum_scatter(part, "ep", scatter_dimension=0, tiled=True)[0].astype(BF16)

        unit = hidden // 6
        part0 = combine(dh1, dh3, unit, 0)
        part0, act_l, ga_l, gb_l = lax.optimization_barrier((part0, act, g_a, g_b))
        out0 = spread(part0)
        keep2, away2 = over_fsdp(dot("pecf,pecd->efd", act_l, ga_l), dot("pecf,pecd->efd", act_l, gb_l))
        away2, d1, d3 = lax.optimization_barrier((away2, dh1, dh3))
        other2 = lax.ppermute(away2, "fsdp", swap)
        part1 = combine(d1, d3, unit, 1)
        part1, d1, d3 = lax.optimization_barrier((part1, d1, d3))
        out1 = spread(part1)
        part2 = combine(d1, d3, 2 * unit, 1)
        part2, d1, d3, x_l = lax.optimization_barrier((part2, d1, d3, x_rows))
        out2 = spread(part2)

        def up_grad(d):
            full = dot("pecd,pecf->edf", x_l, d)
            return over_fsdp(full[:, :half], full[:, half:])

        keep1, away1 = up_grad(d1)
        away1, d3 = lax.optimization_barrier((away1, d3))
        other1 = lax.ppermute(away1, "fsdp", swap)
        keep3, away3 = up_grad(d3)
        away3, d1, d3 = lax.optimization_barrier((away3, d1, d3))
        other3 = lax.ppermute(away3, "fsdp", swap)
        part3 = combine(d1, d3, 2 * unit, 2)
        part3, u_a, u_b = lax.optimization_barrier((part3, u_a, u_b))
        out3 = spread(part3)
        in_grad = jnp.concatenate([out0, out1, out2, out3], axis=-1)

        v = dot("pecd,efd->pecf", u_a, w2a) + dot("pecd,efd->pecf", u_b, w2b)
        slot_dgate = jnp.sum(act.astype(F32) * v, axis=-1)
        spots = jnp.arange(capacity, dtype=I32)
        dense = jnp.sum(jnp.where(place[..., None] == spots, slot_dgate[:, :, None, :], 0.0), axis=-1)
        back = lax.all_to_all(dense, "ep", 0, 0, tiled=True).reshape(experts, tok_dev)
        every = jnp.arange(experts, dtype=I32)[:, None, None]
        gate_out = jnp.sum(jnp.where(expert_ids[None] == every, back[..., None], 0.0), axis=0)
        return in_grad, gate_out, keep1 + other1, keep2 + other2, keep3 + other3

    return jax.shard_map(body, mesh=mesh, in_specs=(tok_spec, tok_spec, tok_spec, tok_spec, up_spec, down_spec, up_spec), out_specs=(tok_spec, tok_spec, up_spec, down_spec, up_spec), check_vma=False)
```
